256 devices in a mesh: tsnk: 16 (over x, z_hi, core), tsrc: 16 (over y, z_lo).
Axes of the slice: x: 4, y: 4, z: 8 (z_hi: 2, z_lo: 4; z = z_hi * 4 + z_lo), core: 2. Of those that a mesh axis runs over, the one named last changes fastest.
Arguments:
- sink_vectors: bfloat16 [16, 2, 256, 3, 13824], P('tsnk', None, None, None, 'tsrc'), may hold values from -0.0546875 to 0.0546875
- source_vectors: bfloat16 [16, 2, 256, 3, 13824], P('tsrc', None, None, None, 'tsnk'), may hold values from -0.0546875 to 0.0546875
- peramb: bfloat16 [16, 16, 4, 2, 256, 4, 256], P('tsnk', 'tsrc'), may hold values from -6 to 6
- momenta: int32 [1, 3], replicated, may hold values from -3 to 3
- sink_times: int32 [16], P('tsnk'), may hold values from 0 to 255
- source_times: int32 [16], P('tsrc'), may hold values from 0 to 255
Outputs:
- correlator: float32 [1, 2, 16, 16], P(None, None, 'tsnk', 'tsrc')
The draws below stay inside these ranges and needn't reach their ends.
All inputs are finite; a program needn't handle non-finite values.
Results may differ from the reference program's by a relative error of at most 0.0055.
Values may be sent and summed in bfloat16 or wider, within the bound.
A program may use at most 128 MiB of HBM per device.

```python
import math
import jax
import jax.numpy as jnp
from jax import lax

VECS = 256
L = 24
COLOURS = 3
SPINS = 4
MOM = 1
TIMES = 256
SITES = 13824
NSNK = 16
NSRC = 16


def place_ends(values, key, low, high):
    spot = [jax.random.randint(jax.random.fold_in(key, axis), (), 0, length) for axis, length in enumerate(values.shape)]
    main_axis = values.shape.index(max(values.shape))
    neighbour = spot[:main_axis] + [(spot[main_axis] + 1) % values.shape[main_axis]] + spot[main_axis + 1:]
    return values.at[tuple(spot)].set(low).at[tuple(neighbour)].set(high)


def level_of(rng, extent, split, low, top_value):
    def one(position, blocks):
        steps = jax.random.uniform(jax.random.fold_in(jax.random.fold_in(rng, 6), position), (blocks,), jnp.float32, low / len(split), top_value / len(split))
        return jnp.repeat(jnp.exp(steps), extent[position] // blocks).reshape((-1,) + (1,) * (len(extent) - position - 1))

    factor_of = one(*split[0])
    for cut in split[1:]:
        factor_of = factor_of * one(*cut)
    return factor_of


def noise(rng, dims, scale, reach, split=(), held_as=jnp.bfloat16):
    entries = jax.random.normal(rng, dims, jnp.float32) * scale
    if len(split) > 0:
        entries = level_of(rng, dims, split, -0.22, 0.18) * entries
    return jnp.clip(entries, min=-reach, max=reach).astype(held_as)


def setup_inputs(seed: int = 0) -> dict:
    arg_keys = jax.random.split(jax.random.key(seed), 7)
    return {
        "sink_vectors": noise(arg_keys[0], (NSNK, 2, VECS, COLOURS, SITES), ((6 * L * L * L) ** -0.5), 0.0546875, ((0, 16), (4, 16))),
        "source_vectors": noise(arg_keys[1], (NSRC, 2, VECS, COLOURS, SITES), ((6 * L * L * L) ** -0.5), 0.0546875, ((0, 16), (4, 16))),
        "peramb": noise(arg_keys[2], (NSNK, NSRC, SPINS, 2, VECS, SPINS, VECS), 0.4, 6.0, ((0, 16), (1, 16))),
        "momenta": jax.random.randint(arg_keys[3], (MOM, 3), -3, 4).astype(jnp.int32),
        "sink_times": place_ends(jax.random.randint(arg_keys[4], (NSNK,), 0, TIMES), jax.random.fold_in(arg_keys[4], 1), 0, TIMES - 1).astype(jnp.int32),
        "source_times": place_ends(jax.random.randint(arg_keys[5], (NSRC,), 0, TIMES), jax.random.fold_in(arg_keys[5], 1), 0, TIMES - 1).astype(jnp.int32),
    }


GAMMA_FIVE = (1.0, 1.0, -1.0, -1.0)


def phase_table(momenta):
    site_index = jnp.arange(L * L * L, dtype=jnp.int32)
    coord_x = site_index // (L * L)
    coord_y = (site_index // L) % L
    coord_z = site_index % L
    winding = (momenta[:, 0:1] * coord_x[None, :] + momenta[:, 1:2] * coord_y[None, :] + momenta[:, 2:3] * coord_z[None, :]) % L
    angle = winding.astype(jnp.float32) * (2.0 * math.pi / L)
    return jnp.cos(angle), jnp.sin(angle)


def elemental_slice(vectors, cosine, sine):
    vec_real = vectors[0]
    vec_imag = vectors[1]
    left = jnp.concatenate([vec_real.reshape(VECS, -1), vec_imag.reshape(VECS, -1)], 1)
    outputs = []
    for moment in range(MOM):
        cos_m = cosine[moment][None, None, :]
        sin_m = sine[moment][None, None, :]
        wave_real = (cos_m * vec_real.astype(jnp.float32) - sin_m * vec_imag.astype(jnp.float32)).astype(jnp.bfloat16).reshape(VECS, -1)
        wave_imag = (cos_m * vec_imag.astype(jnp.float32) + sin_m * vec_real.astype(jnp.float32)).astype(jnp.bfloat16).reshape(VECS, -1)
        right = jnp.concatenate([jnp.concatenate([wave_real, wave_imag], 1), jnp.concatenate([wave_imag, -wave_real], 1)], 0)
        product = jnp.dot(left, right.T, preferred_element_type=jnp.float32)
        outputs.append(product.reshape(VECS, 2, VECS))
    return jnp.stack(outputs, 1).astype(jnp.bfloat16)


def pair_value(sink_elem, source_elem, perm):
    gamma_five = jnp.array(GAMMA_FIVE, dtype=jnp.float32)
    signs = (-(gamma_five[:, None] * gamma_five[None, :]))[:, None, :, None]
    order = jnp.array([2, 3, 0, 1], dtype=jnp.int32)
    peram_real = perm[:, 0].astype(jnp.float32)
    peram_imag = perm[:, 1].astype(jnp.float32)
    swap_real = peram_real[order]
    swap_imag = peram_imag[order]
    values = []
    for moment in range(MOM):
        sink_real = sink_elem[:, moment, 0].astype(jnp.float32)
        sink_imag = sink_elem[:, moment, 1].astype(jnp.float32)
        src_real = source_elem[:, moment, 0].astype(jnp.float32)
        src_imag = source_elem[:, moment, 1].astype(jnp.float32)
        left_real = jnp.einsum('ab,sbtc->satc', sink_real, swap_real) - jnp.einsum('ab,sbtc->satc', sink_imag, swap_imag)
        left_imag = jnp.einsum('ab,sbtc->satc', sink_real, swap_imag) + jnp.einsum('ab,sbtc->satc', sink_imag, swap_real)
        right_real = jnp.einsum('satb,bc->satc', peram_real, src_real) - jnp.einsum('satb,bc->satc', peram_imag, src_imag)
        right_imag = jnp.einsum('satb,bc->satc', peram_real, src_imag) + jnp.einsum('satb,bc->satc', peram_imag, src_real)
        right_real = right_real[:, :, order]
        right_imag = right_imag[:, :, order]
        value_real = jnp.sum(signs * (left_real * right_real + left_imag * right_imag))
        value_imag = jnp.sum(signs * (left_imag * right_real - left_real * right_imag))
        values.append(jnp.stack([value_real, value_imag]))
    return jnp.stack(values)


def reference(sink_vectors, source_vectors, peramb, momenta, sink_times, source_times):
    cosine, sine = phase_table(momenta)
    sink_elems = lax.map(lambda vectors: elemental_slice(vectors, cosine, sine), sink_vectors)
    source_elems = lax.map(lambda vectors: elemental_slice(vectors, cosine, sine), source_vectors)
    pair_index = jnp.arange(NSNK * NSRC, dtype=jnp.int32)

    def one_pair(pair):
        sink_row = pair // NSRC
        source_col = pair % NSRC
        value = pair_value(sink_elems[sink_row], source_elems[source_col], peramb[sink_row, source_col])
        keep = (sink_times[sink_row] >= source_times[source_col]).astype(jnp.float32)
        return value * keep

    values = lax.map(one_pair, pair_index)
    return jnp.transpose(values.reshape(NSNK, NSRC, MOM, 2), (2, 3, 0, 1))
```

```python
import math

import jax
import jax.numpy as jnp
from jax import lax
from jax.experimental import pallas as pl
from jax.experimental.pallas import tpu as pltpu
from jax.sharding import PartitionSpec as P

VECS = 256
L = 24
SITES = 864
COLOURS = 3
MESH = pl.DeviceIdType.MESH
COS = [math.cos(2.0 * math.pi * k / L) for k in range(L)]
SIN = [math.sin(2.0 * math.pi * k / L) for k in range(L)]


def mod_winding(v):
    return v - 24.0 * jnp.floor((v + 0.5) * (1.0 / 24.0))


def cos_sin(k):
    cosine = jnp.zeros_like(k)
    sine = jnp.zeros_like(k)
    for m in range(L):
        hit = k == float(m)
        cosine = jnp.where(hit, COS[m], cosine)
        sine = jnp.where(hit, SIN[m], sine)
    return cosine, sine


def phase_tables(mom_ref, first_row, cos_ref, sin_ref):
    px = mom_ref[0, 0].astype(jnp.float32)
    py = mom_ref[0, 1].astype(jnp.float32)
    pz = mom_ref[0, 2].astype(jnp.float32)
    z = lax.broadcasted_iota(jnp.int32, (L, 128), 0).astype(jnp.float32)
    cos_z, sin_z = cos_sin(mod_winding(pz * z))
    row = (lax.broadcasted_iota(jnp.int32, (40, 128), 0) + first_row).astype(jnp.float32)
    x = jnp.floor((row + 0.5) * (1.0 / L))
    y = row - L * x
    cos_q, sin_q = cos_sin(mod_winding(px * x + py * y))
    for q in range(SITES // L):
        cq = jnp.broadcast_to(cos_q[q : q + 1, :], (L, 128))
        sq = jnp.broadcast_to(sin_q[q : q + 1, :], (L, 128))
        cos_ref[q * L : (q + 1) * L, :] = cq * cos_z - sq * sin_z
        sin_ref[q * L : (q + 1) * L, :] = sq * cos_z + cq * sin_z


def partial_elemental(colour_copies, vec_ref, wave_ref, cos_ref, sin_ref, acc_ref, out_ref):
    rows = 96
    for colour in range(COLOURS):
        for copy in colour_copies[colour]:
            copy.wait()

        def block(step, carry):
            at = pl.ds(pl.multiple_of(step * rows, rows), rows)
            cosine = cos_ref[at, :]
            sine = sin_ref[at, :]
            for half in range(2):
                lanes = pl.ds(half * 128, 128)
                lanes_imag = pl.ds(256 + half * 128, 128)
                real = vec_ref[colour, at, lanes].astype(jnp.float32)
                imag = vec_ref[colour, at, lanes_imag].astype(jnp.float32)
                wave_ref[colour, at, lanes] = (cosine * real - sine * imag).astype(jnp.bfloat16)
                wave_ref[colour, at, lanes_imag] = (cosine * imag + sine * real).astype(jnp.bfloat16)
            return carry

        lax.fori_loop(0, SITES // rows, block, 0)
        term = lax.dot_general(
            vec_ref[colour], wave_ref[colour], (((0,), (0,)), ((), ())), preferred_element_type=jnp.float32
        )
        if colour == 0:
            acc_ref[...] = term
        elif colour < COLOURS - 1:
            acc_ref[...] += term
        else:
            term = term + acc_ref[...]
            out_ref[:, 0:256] = term[0:256, 0:256] + term[256:512, 256:512]
            out_ref[:, 256:512] = term[0:256, 256:512] - term[256:512, 0:256]


def kernel(
    sink_hbm, source_hbm, per_hbm, mom_ref, snk_t, src_t,
    out_ref,
    snk_vec, src_vec, wave, cos_ref, sin_ref, acc,
    snk_part, src_part, per, pt, tbuf,
    y_recv, y_sum, z_recv, elem, core_recv, core_sum, x_recv, x_sum, zz_recv, src_elem,
    est, sst, tot,
    load_sem, send_sem, recv_sem,
):
    i = lax.axis_index("tsnk")
    j = lax.axis_index("tsrc")
    x, zh, c = i // 4, (i // 2) % 2, i % 2
    y, zl = j // 4, j % 4
    core_peer = (4 * x + 2 * zh + (1 - c), j)
    z_peer = (4 * x + 2 * (1 - zh) + c, j)
    x_peers = [(4 * ((x + d) % 4) + 2 * zh + c, j) for d in (1, 2, 3)]
    y_peers = [(i, 4 * ((y + d) % 4) + zl) for d in (1, 2, 3)]
    zl_peers = [(i, 4 * y + (zl + d) % 4) for d in (1, 2, 3)]

    def load(n, src, dst):
        copy = pltpu.make_async_copy(src, dst, load_sem.at[n])
        copy.start()
        return copy

    snk_loads = [
        [load(2 * k + r, sink_hbm.at[r, k], snk_vec.at[k, :, pl.ds(r * 256, 256)]) for r in range(2)]
        for k in range(COLOURS)
    ]
    src_loads = [
        [load(6 + 2 * k + r, source_hbm.at[r, k], src_vec.at[k, :, pl.ds(r * 256, 256)]) for r in range(2)]
        for k in range(COLOURS)
    ]
    per_loads = [load(12 + s, per_hbm.at[s], per.at[s]) for s in range(4)]

    barrier = pltpu.get_barrier_semaphore()
    peers = [core_peer, z_peer] + x_peers + y_peers + zl_peers
    for peer in peers:
        pl.semaphore_signal(barrier, inc=1, device_id=peer, device_id_type=MESH)

    def remote(n, src, dst, peer):
        return pltpu.make_async_remote_copy(
            src_ref=src, dst_ref=dst, send_sem=send_sem.at[n], recv_sem=recv_sem.at[n],
            device_id=peer, device_id_type=MESH,
        )

    def start(copies):
        for copy in copies:
            copy.start()

    phase_tables(mom_ref, j * (SITES // L), cos_ref, sin_ref)
    partial_elemental(snk_loads, snk_vec, wave, cos_ref, sin_ref, acc, snk_part)
    pl.semaphore_wait(barrier, len(peers))
    sent = []

    def block_of(start_row, size):
        return pl.ds(pl.multiple_of(start_row, size), size)

    y_rs = [
        remote(d, snk_part.at[block_of(64 * ((y + d + 1) % 4), 64)], y_recv.at[d], y_peers[d]) for d in range(3)
    ]
    start(y_rs)

    phase_tables(mom_ref, i * (SITES // L), cos_ref, sin_ref)
    partial_elemental(src_loads, src_vec, wave, cos_ref, sin_ref, acc, src_part)
    core_rs = remote(3, src_part.at[block_of(128 * (1 - c), 128)], core_recv, core_peer)
    core_rs.start()

    out_row = lax.broadcasted_iota(jnp.int32, (256, 256), 0)
    in_row = lax.broadcasted_iota(jnp.int32, (256, 256), 1)
    pick = jnp.where((out_row % 32) * 8 + out_row // 32 == in_row, 1.0, 0.0).astype(jnp.bfloat16)

    def unmix(s, carry):
        per_loads_wait = pltpu.make_async_copy(per_hbm.at[s], per.at[s], load_sem.at[12 + s])
        per_loads_wait.wait()
        for blk in range(8):
            rows = pl.ds(blk * 256, 256)
            both = jnp.concatenate([per[s, 0, rows, :], per[s, 1, rows, :]], axis=1)
            moved = jnp.dot(pick, both, preferred_element_type=jnp.float32).astype(jnp.bfloat16)
            for t in range(4):
                for half in range(2):
                    piece = moved[(half * 4 + t) * 32 : (half * 4 + t + 1) * 32, :]
                    for r in range(2):
                        pt[s, t, pl.ds(blk * 32, 32), pl.ds(r * 256 + half * 128, 128)] = piece[
                            :, r * 128 : (r + 1) * 128
                        ]
        return carry

    lax.fori_loop(0, 2, unmix, 0)
    core_rs.wait_recv()
    core_sum[...] = src_part[block_of(128 * c, 128), :] + core_recv[...]
    x_rs = [
        remote(4 + d, core_sum.at[block_of(32 * ((x + d + 1) % 4), 32)], x_recv.at[d], x_peers[d]) for d in range(3)
    ]
    start(x_rs)
    lax.fori_loop(2, 4, unmix, 0)

    for copy in y_rs:
        copy.wait_recv()
    y_sum[...] = (snk_part[block_of(64 * y, 64), :] + y_recv[0]) + (y_recv[1] + y_recv[2])
    z_rs = [
        remote(7 + d, y_sum.at[block_of(16 * ((zl + d + 1) % 4), 16)], z_recv.at[d], zl_peers[d]) for d in range(3)
    ]
    start(z_rs)

    for copy in x_rs:
        copy.wait_recv()
    x_sum[...] = (core_sum[block_of(32 * x, 32), :] + x_recv[0]) + (x_recv[1] + x_recv[2])
    zz = remote(10, x_sum, zz_recv, z_peer)
    zz.start()

    for copy in z_rs:
        copy.wait_recv()
    mine = (y_sum[block_of(16 * zl, 16), :] + z_recv[0]) + (z_recv[1] + z_recv[2])
    own = elem.at[block_of(64 * y + 16 * zl, 16)]
    own[...] = mine.astype(jnp.bfloat16)
    z_ag = [remote(11 + d, own, own, zl_peers[d]) for d in range(3)]
    start(z_ag)
    y_ag = [remote(14 + d, own, own, y_peers[d]) for d in range(3)]
    start(y_ag)

    zz.wait_recv()
    src_own = src_elem.at[block_of(128 * c + 32 * x, 32)]
    src_own[...] = (x_sum[...] + zz_recv[...]).astype(jnp.bfloat16)
    x_ag = [remote(26 + d, src_own, src_own, x_peers[d]) for d in range(3)]
    start(x_ag)
    core_ag = [remote(29, src_own, src_own, core_peer)]
    start(core_ag)

    for d in range(3):
        z_ag[d].wait_recv()
        came = elem.at[block_of(64 * y + 16 * ((zl + 3 - d) % 4), 16)]
        onward = [remote(17 + 3 * d + e, came, came, y_peers[e]) for e in range(3)]
        start(onward)
        y_ag += onward
    for d in range(3):
        x_ag[d].wait_recv()
        came = src_elem.at[block_of(128 * c + 32 * ((x + 3 - d) % 4), 32)]
        onward = remote(30 + d, came, came, core_peer)
        onward.start()
        core_ag.append(onward)
    for copy in core_ag:
        copy.wait_recv()

    sst[0:256, :] = src_elem[...]
    sst[256:512, 0:256] = -src_elem[:, 256:512]
    sst[256:512, 256:512] = src_elem[:, 0:256]

    def right(s, carry):
        for t in range(4):
            tbuf[s, t] = jnp.dot(pt[s, t], sst[...], preferred_element_type=jnp.float32)
        return carry

    lax.fori_loop(0, 4, right, 0)

    for copy in y_ag:
        copy.wait_recv()
    est[0:256, 0:256] = elem[:, 0:256]
    est[0:256, 256:512] = -elem[:, 256:512]
    est[256:512, 0:256] = elem[:, 256:512]
    est[256:512, 256:512] = elem[:, 0:256]
    tot[...] = jnp.zeros_like(tot)

    def fold(v):
        return v.reshape(32, 8, 256).sum(axis=0)

    def left(s, carry):
        other = (s + 2) % 4
        sum_real = jnp.zeros((8, 256), jnp.float32)
        sum_imag = jnp.zeros((8, 256), jnp.float32)
        for t in range(4):
            lt = jnp.dot(est[:, 0:256], pt[s, t, :, 0:256], preferred_element_type=jnp.float32)
            lt = lt + jnp.dot(est[:, 256:512], pt[s, t, :, 256:512], preferred_element_type=jnp.float32)
            right_real = tbuf[other, t ^ 2, :, 0:256]
            right_imag = tbuf[other, t ^ 2, :, 256:512]
            left_real = lt[0:256]
            left_imag = lt[256:512]
            real = fold(left_real * right_real + left_imag * right_imag)
            imag = fold(left_imag * right_real - left_real * right_imag)
            if t < 2:
                sum_real, sum_imag = sum_real + real, sum_imag + imag
            else:
                sum_real, sum_imag = sum_real - real, sum_imag - imag
        sign = 1.0 - 2.0 * (s // 2).astype(jnp.float32)
        tot[0] += sign * sum_real
        tot[1] += sign * sum_imag
        return carry

    lax.fori_loop(0, 4, left, 0)
    keep = jnp.where(snk_t[0] >= src_t[0], 1.0, 0.0)
    out_ref[0, 0] = jnp.sum(tot[0]) * keep
    out_ref[0, 1] = jnp.sum(tot[1]) * keep

    for copy in y_rs + [core_rs] + x_rs + z_rs + [zz] + z_ag + y_ag + x_ag + core_ag:
        copy.wait_send()


def per_device(sink_vectors, source_vectors, peramb, momenta, sink_times, source_times):
    sink = sink_vectors[0].transpose(0, 2, 3, 1)
    source = source_vectors[0].transpose(0, 2, 3, 1)
    per = peramb[0, 0].reshape(4, 2, 256, 4, 2, 128).transpose(0, 1, 2, 4, 3, 5).reshape(4, 2, 2048, 128)
    hbm = pl.BlockSpec(memory_space=pl.ANY)
    smem = pl.BlockSpec(memory_space=pltpu.SMEM)
    f32, bf16 = jnp.float32, jnp.bfloat16
    values = pl.pallas_call(
        kernel,
        out_shape=jax.ShapeDtypeStruct((1, 2), f32),
        in_specs=[hbm, hbm, hbm, smem, smem, smem],
        out_specs=smem,
        scratch_shapes=[
            pltpu.VMEM((COLOURS, SITES, 512), bf16),
            pltpu.VMEM((COLOURS, SITES, 512), bf16),
            pltpu.VMEM((COLOURS, SITES, 512), bf16),
            pltpu.VMEM((SITES, 128), f32),
            pltpu.VMEM((SITES, 128), f32),
            pltpu.VMEM((512, 512), f32),
            pltpu.VMEM((256, 512), f32),
            pltpu.VMEM((256, 512), f32),
            pltpu.VMEM((4, 2, 2048, 128), bf16),
            pltpu.VMEM((4, 4, 256, 512), bf16),
            pltpu.VMEM((4, 4, 256, 512), f32),
            pltpu.VMEM((3, 64, 512), f32),
            pltpu.VMEM((64, 512), f32),
            pltpu.VMEM((3, 16, 512), f32),
            pltpu.VMEM((256, 512), bf16),
            pltpu.VMEM((128, 512), f32),
            pltpu.VMEM((128, 512), f32),
            pltpu.VMEM((3, 32, 512), f32),
            pltpu.VMEM((32, 512), f32),
            pltpu.VMEM((32, 512), f32),
            pltpu.VMEM((256, 512), bf16),
            pltpu.VMEM((512, 512), bf16),
            pltpu.VMEM((512, 512), bf16),
            pltpu.VMEM((2, 8, 256), f32),
            pltpu.SemaphoreType.DMA((16,)),
            pltpu.SemaphoreType.DMA((33,)),
            pltpu.SemaphoreType.DMA((33,)),
        ],
        compiler_params=pltpu.CompilerParams(
            collective_id=0, has_side_effects=True, vmem_limit_bytes=60 * 1024 * 1024
        ),
    )(sink, source, per, momenta, sink_times, source_times)
    return values.reshape(1, 2, 1, 1)


def solution(mesh):
    return jax.shard_map(
        per_device,
        mesh=mesh,
        in_specs=(
            P("tsnk", None, None, None, "tsrc"),
            P("tsrc", None, None, None, "tsnk"),
            P("tsnk", "tsrc", None, None, None, None, None),
            P(),
            P("tsnk"),
            P("tsrc"),
        ),
        out_specs=P(None, None, "tsnk", "tsrc"),
        check_vma=False,
    )
```

```python
import math

import jax
import jax.numpy as jnp
from jax import lax
from jax.experimental import pallas as pl
from jax.experimental.pallas import tpu as pltpu
from jax.sharding import PartitionSpec as P

VECS = 256
L = 24
SITES = 864
COLOURS = 3
MESH = pl.DeviceIdType.MESH
COS = [math.cos(2.0 * math.pi * k / L) for k in range(L)]
SIN = [math.sin(2.0 * math.pi * k / L) for k in range(L)]


def mod_winding(v):
    return v - 24.0 * jnp.floor((v + 0.5) * (1.0 / 24.0))


def cos_sin(k):
    cosine = jnp.zeros_like(k)
    sine = jnp.zeros_like(k)
    for m in range(L):
        hit = k == float(m)
        cosine = jnp.where(hit, COS[m], cosine)
        sine = jnp.where(hit, SIN[m], sine)
    return cosine, sine


def phase_tables(mom_ref, first_row, cos_ref, sin_ref):
    px = mom_ref[0, 0].astype(jnp.float32)
    py = mom_ref[0, 1].astype(jnp.float32)
    pz = mom_ref[0, 2].astype(jnp.float32)
    z = lax.broadcasted_iota(jnp.int32, (L, 128), 0).astype(jnp.float32)
    cos_z, sin_z = cos_sin(mod_winding(pz * z))
    row = (lax.broadcasted_iota(jnp.int32, (40, 128), 0) + first_row).astype(jnp.float32)
    x = jnp.floor((row + 0.5) * (1.0 / L))
    y = row - L * x
    cos_q, sin_q = cos_sin(mod_winding(px * x + py * y))
    for q in range(SITES // L):
        cq = jnp.broadcast_to(cos_q[q : q + 1, :], (L, 128))
        sq = jnp.broadcast_to(sin_q[q : q + 1, :], (L, 128))
        cos_ref[q * L : (q + 1) * L, :] = cq * cos_z - sq * sin_z
        sin_ref[q * L : (q + 1) * L, :] = sq * cos_z + cq * sin_z


def wave_of(colour, vec_ref, wave_ref, cos_ref, sin_ref):
    rows = 48
    for step in range(SITES // rows):
        at = pl.ds(step * rows, rows)
        cosine = cos_ref[at, :]
        sine = sin_ref[at, :]
        for half in range(2):
            lanes = pl.ds(half * 128, 128)
            lanes_imag = pl.ds(256 + half * 128, 128)
            real = vec_ref[colour, at, lanes].astype(jnp.float32)
            imag = vec_ref[colour, at, lanes_imag].astype(jnp.float32)
            wave_ref[colour, at, lanes] = (cosine * real - sine * imag).astype(jnp.bfloat16)
            wave_ref[colour, at, lanes_imag] = (cosine * imag + sine * real).astype(jnp.bfloat16)


def colour_term(colour, vec_ref, wave_ref):
    return lax.dot_general(
        vec_ref[colour], wave_ref[colour], (((0,), (0,)), ((), ())), preferred_element_type=jnp.float32
    )


def finish_elemental(term, out_ref):
    out_ref[:, 0:256] = term[0:256, 0:256] + term[256:512, 256:512]
    out_ref[:, 256:512] = term[0:256, 256:512] - term[256:512, 0:256]


def kernel(
    sink_hbm, source_hbm, per_hbm, mom_ref, snk_t, src_t,
    out_ref,
    snk_vec, src_vec, wave, wave2, cos_ref, sin_ref, acc,
    snk_part, src_part, per, pt, tbuf,
    y_recv, y_sum, z_recv, elem, core_recv, core_sum, x_recv, x_sum, zz_recv, src_elem,
    est, sst, tot,
    load_sem, send_sem, recv_sem,
):
    i = lax.axis_index("tsnk")
    j = lax.axis_index("tsrc")
    x, zh, c = i // 4, (i // 2) % 2, i % 2
    y, zl = j // 4, j % 4
    core_peer = (4 * x + 2 * zh + (1 - c), j)
    z_peer = (4 * x + 2 * (1 - zh) + c, j)
    x_peers = [(4 * ((x + d) % 4) + 2 * zh + c, j) for d in (1, 2, 3)]
    y_peers = [(i, 4 * ((y + d) % 4) + zl) for d in (1, 2, 3)]
    zl_peers = [(i, 4 * y + (zl + d) % 4) for d in (1, 2, 3)]

    def load(n, src, dst):
        copy = pltpu.make_async_copy(src, dst, load_sem.at[n])
        copy.start()
        return copy

    src_loads = [
        [load(6 + 2 * k + r, source_hbm.at[r, k], src_vec.at[k, :, pl.ds(r * 256, 256)]) for r in range(2)]
        for k in range(COLOURS)
    ]
    snk_loads = [
        [load(2 * k + r, sink_hbm.at[r, k], snk_vec.at[k, :, pl.ds(r * 256, 256)]) for r in range(2)]
        for k in range(COLOURS)
    ]
    per_loads = [load(12 + s, per_hbm.at[s], per.at[s]) for s in range(4)]

    barrier = pltpu.get_barrier_semaphore()
    peers = [core_peer, z_peer] + x_peers + y_peers + zl_peers
    for peer in peers:
        pl.semaphore_signal(barrier, inc=1, device_id=peer, device_id_type=MESH)

    def remote(n, src, dst, peer):
        return pltpu.make_async_remote_copy(
            src_ref=src, dst_ref=dst, send_sem=send_sem.at[n], recv_sem=recv_sem.at[n],
            device_id=peer, device_id_type=MESH,
        )

    def start(copies):
        for copy in copies:
            copy.start()

    def block_of(start_row, size):
        return pl.ds(pl.multiple_of(start_row, size), size)

    def loaded(copies):
        for copy in copies:
            copy.wait()

    phase_tables(mom_ref, i * (SITES // L), cos_ref, sin_ref)
    loaded(src_loads[0])
    wave_of(0, src_vec, wave, cos_ref, sin_ref)
    loaded(src_loads[1])
    acc[...] = colour_term(0, src_vec, wave)
    wave_of(1, src_vec, wave, cos_ref, sin_ref)
    loaded(src_loads[2])
    acc[...] += colour_term(1, src_vec, wave)
    wave_of(2, src_vec, wave, cos_ref, sin_ref)
    finish_elemental(acc[...] + colour_term(2, src_vec, wave), src_part)
    pl.semaphore_wait(barrier, len(peers))
    core_rs = remote(3, src_part.at[block_of(128 * (1 - c), 128)], core_recv, core_peer)
    core_rs.start()

    phase_tables(mom_ref, j * (SITES // L), cos_ref, sin_ref)
    for colour in range(COLOURS):
        loaded(snk_loads[colour])
    wave_of(0, snk_vec, wave2, cos_ref, sin_ref)
    acc[...] = colour_term(0, snk_vec, wave2)
    wave_of(1, snk_vec, wave2, cos_ref, sin_ref)
    core_rs.wait_recv()
    core_sum[...] = src_part[block_of(128 * c, 128), :] + core_recv[...]
    x_rs = [
        remote(4 + d, core_sum.at[block_of(32 * ((x + d + 1) % 4), 32)], x_recv.at[d], x_peers[d]) for d in range(3)
    ]
    start(x_rs)
    acc[...] += colour_term(1, snk_vec, wave2)
    wave_of(2, snk_vec, wave2, cos_ref, sin_ref)
    finish_elemental(acc[...] + colour_term(2, snk_vec, wave2), snk_part)
    y_rs = [
        remote(d, snk_part.at[block_of(64 * ((y + d + 1) % 4), 64)], y_recv.at[d], y_peers[d]) for d in range(3)
    ]
    start(y_rs)

    out_row = lax.broadcasted_iota(jnp.int32, (256, 256), 0)
    in_row = lax.broadcasted_iota(jnp.int32, (256, 256), 1)
    pick = jnp.where((out_row % 32) * 8 + out_row // 32 == in_row, 1.0, 0.0).astype(jnp.bfloat16)

    def unmix(s, carry):
        per_loads_wait = pltpu.make_async_copy(per_hbm.at[s], per.at[s], load_sem.at[12 + s])
        per_loads_wait.wait()
        for blk in range(8):
            rows = pl.ds(blk * 256, 256)
            both = jnp.concatenate([per[s, 0, rows, :], per[s, 1, rows, :]], axis=1)
            moved = jnp.dot(pick, both, preferred_element_type=jnp.float32).astype(jnp.bfloat16)
            for t in range(4):
                for half in range(2):
                    piece = moved[(half * 4 + t) * 32 : (half * 4 + t + 1) * 32, :]
                    for r in range(2):
                        pt[s, t, r, pl.ds(blk * 32, 32), pl.ds(half * 128, 128)] = piece[
                            :, r * 128 : (r + 1) * 128
                        ]
        return carry

    lax.fori_loop(0, 4, unmix, 0)

    for copy in x_rs:
        copy.wait_recv()
    x_sum[...] = (core_sum[block_of(32 * x, 32), :] + x_recv[0]) + (x_recv[1] + x_recv[2])
    zz = remote(10, x_sum, zz_recv, z_peer)
    zz.start()

    for copy in y_rs:
        copy.wait_recv()
    y_sum[...] = (snk_part[block_of(64 * y, 64), :] + y_recv[0]) + (y_recv[1] + y_recv[2])
    z_rs = [
        remote(7 + d, y_sum.at[block_of(16 * ((zl + d + 1) % 4), 16)], z_recv.at[d], zl_peers[d]) for d in range(3)
    ]
    start(z_rs)

    zz.wait_recv()
    src_own = src_elem.at[block_of(128 * c + 32 * x, 32)]
    src_own[...] = (x_sum[...] + zz_recv[...]).astype(jnp.bfloat16)
    x_ag = [remote(26 + d, src_own, src_own, x_peers[d]) for d in range(3)]
    start(x_ag)
    core_ag = [remote(29, src_own, src_own, core_peer)]
    start(core_ag)

    for copy in z_rs:
        copy.wait_recv()
    mine = (y_sum[block_of(16 * zl, 16), :] + z_recv[0]) + (z_recv[1] + z_recv[2])
    own = elem.at[block_of(64 * y + 16 * zl, 16)]
    own[...] = mine.astype(jnp.bfloat16)
    z_ag = [remote(11 + d, own, own, zl_peers[d]) for d in range(3)]
    start(z_ag)
    y_ag = [remote(14 + d, own, own, y_peers[d]) for d in range(3)]
    start(y_ag)

    for d in range(3):
        x_ag[d].wait_recv()
        came = src_elem.at[block_of(128 * c + 32 * ((x + 3 - d) % 4), 32)]
        onward = remote(30 + d, came, came, core_peer)
        onward.start()
        core_ag.append(onward)
    for d in range(3):
        z_ag[d].wait_recv()
        came = elem.at[block_of(64 * y + 16 * ((zl + 3 - d) % 4), 16)]
        onward = [remote(17 + 3 * d + e, came, came, y_peers[e]) for e in range(3)]
        start(onward)
        y_ag += onward
    for copy in core_ag:
        copy.wait_recv()

    sst[0:256, :] = src_elem[...]
    sst[256:512, 0:256] = -src_elem[:, 256:512]
    sst[256:512, 256:512] = src_elem[:, 0:256]

    def right(s, carry):
        for t in range(4):
            rows = jnp.concatenate([pt[s, t, 0], pt[s, t, 1]], axis=1)
            tbuf[s, t] = jnp.dot(rows, sst[...], preferred_element_type=jnp.float32)
        return carry

    lax.fori_loop(0, 4, right, 0)

    for copy in y_ag:
        copy.wait_recv()
    est[0:256, 0:256] = elem[:, 0:256]
    est[0:256, 256:512] = -elem[:, 256:512]
    est[256:512, 0:256] = elem[:, 256:512]
    est[256:512, 256:512] = elem[:, 0:256]
    tot[...] = jnp.zeros_like(tot)

    def fold(v):
        return v.reshape(32, 8, 256).sum(axis=0)

    def left(s, carry):
        other = (s + 2) % 4
        sum_real = jnp.zeros((8, 256), jnp.float32)
        sum_imag = jnp.zeros((8, 256), jnp.float32)
        for t in range(4):
            lt = jnp.dot(est[...], pt[s, t].reshape(512, 256), preferred_element_type=jnp.float32)
            right_real = tbuf[other, t ^ 2, :, 0:256]
            right_imag = tbuf[other, t ^ 2, :, 256:512]
            left_real = lt[0:256]
            left_imag = lt[256:512]
            real = fold(left_real * right_real + left_imag * right_imag)
            imag = fold(left_imag * right_real - left_real * right_imag)
            if t < 2:
                sum_real, sum_imag = sum_real + real, sum_imag + imag
            else:
                sum_real, sum_imag = sum_real - real, sum_imag - imag
        sign = 1.0 - 2.0 * (s // 2).astype(jnp.float32)
        tot[0] += sign * sum_real
        tot[1] += sign * sum_imag
        return carry

    lax.fori_loop(0, 4, left, 0)
    keep = jnp.where(snk_t[0] >= src_t[0], 1.0, 0.0)
    out_ref[0, 0] = jnp.sum(tot[0]) * keep
    out_ref[0, 1] = jnp.sum(tot[1]) * keep

    for copy in y_rs + [core_rs] + x_rs + z_rs + [zz] + z_ag + y_ag + x_ag + core_ag:
        copy.wait_send()


def per_device(sink_vectors, source_vectors, peramb, momenta, sink_times, source_times):
    sink = sink_vectors[0].transpose(0, 2, 3, 1)
    source = source_vectors[0].transpose(0, 2, 3, 1)
    per = peramb[0, 0].reshape(4, 2, 256, 4, 2, 128).transpose(0, 1, 2, 4, 3, 5).reshape(4, 2, 2048, 128)
    hbm = pl.BlockSpec(memory_space=pl.ANY)
    smem = pl.BlockSpec(memory_space=pltpu.SMEM)
    f32, bf16 = jnp.float32, jnp.bfloat16
    values = pl.pallas_call(
        kernel,
        out_shape=jax.ShapeDtypeStruct((1, 2), f32),
        in_specs=[hbm, hbm, hbm, smem, smem, smem],
        out_specs=smem,
        scratch_shapes=[
            pltpu.VMEM((COLOURS, SITES, 512), bf16),
            pltpu.VMEM((COLOURS, SITES, 512), bf16),
            pltpu.VMEM((COLOURS, SITES, 512), bf16),
            pltpu.VMEM((COLOURS, SITES, 512), bf16),
            pltpu.VMEM((SITES, 128), f32),
            pltpu.VMEM((SITES, 128), f32),
            pltpu.VMEM((512, 512), f32),
            pltpu.VMEM((256, 512), f32),
            pltpu.VMEM((256, 512), f32),
            pltpu.VMEM((4, 2, 2048, 128), bf16),
            pltpu.VMEM((4, 4, 2, 256, 256), bf16),
            pltpu.VMEM((4, 4, 256, 512), f32),
            pltpu.VMEM((3, 64, 512), f32),
            pltpu.VMEM((64, 512), f32),
            pltpu.VMEM((3, 16, 512), f32),
            pltpu.VMEM((256, 512), bf16),
            pltpu.VMEM((128, 512), f32),
            pltpu.VMEM((128, 512), f32),
            pltpu.VMEM((3, 32, 512), f32),
            pltpu.VMEM((32, 512), f32),
            pltpu.VMEM((32, 512), f32),
            pltpu.VMEM((256, 512), bf16),
            pltpu.VMEM((512, 512), bf16),
            pltpu.VMEM((512, 512), bf16),
            pltpu.VMEM((2, 8, 256), f32),
            pltpu.SemaphoreType.DMA((16,)),
            pltpu.SemaphoreType.DMA((33,)),
            pltpu.SemaphoreType.DMA((33,)),
        ],
        compiler_params=pltpu.CompilerParams(
            collective_id=0, has_side_effects=True, vmem_limit_bytes=60 * 1024 * 1024
        ),
    )(sink, source, per, momenta, sink_times, source_times)
    return values.reshape(1, 2, 1, 1)


def solution(mesh):
    return jax.shard_map(
        per_device,
        mesh=mesh,
        in_specs=(
            P("tsnk", None, None, None, "tsrc"),
            P("tsrc", None, None, None, "tsnk"),
            P("tsnk", "tsrc", None, None, None, None, None),
            P(),
            P("tsnk"),
            P("tsrc"),
        ),
        out_specs=P(None, None, "tsnk", "tsrc"),
        check_vma=False,
    )
```

```python
import math

import jax
import jax.numpy as jnp
from jax import lax
from jax.experimental import pallas as pl
from jax.experimental.pallas import tpu as pltpu
from jax.sharding import PartitionSpec as P

VECS = 256
L = 24
SITES = 864
COLOURS = 3
MESH = pl.DeviceIdType.MESH
COS = [math.cos(2.0 * math.pi * k / L) for k in range(L)]
SIN = [math.sin(2.0 * math.pi * k / L) for k in range(L)]


def mod_winding(v):
    return v - 24.0 * jnp.floor((v + 0.5) * (1.0 / 24.0))


def cos_sin(k):
    cosine = jnp.zeros_like(k)
    sine = jnp.zeros_like(k)
    for m in range(L):
        hit = k == float(m)
        cosine = jnp.where(hit, COS[m], cosine)
        sine = jnp.where(hit, SIN[m], sine)
    return cosine, sine


def phase_tables(mom_ref, first_row, cos_ref, sin_ref):
    px = mom_ref[0, 0].astype(jnp.float32)
    py = mom_ref[0, 1].astype(jnp.float32)
    pz = mom_ref[0, 2].astype(jnp.float32)
    z = lax.broadcasted_iota(jnp.int32, (L, 128), 0).astype(jnp.float32)
    cos_z, sin_z = cos_sin(mod_winding(pz * z))
    row = (lax.broadcasted_iota(jnp.int32, (40, 128), 0) + first_row).astype(jnp.float32)
    x = jnp.floor((row + 0.5) * (1.0 / L))
    y = row - L * x
    cos_q, sin_q = cos_sin(mod_winding(px * x + py * y))
    for q in range(SITES // L):
        cq = jnp.broadcast_to(cos_q[q : q + 1, :], (L, 128))
        sq = jnp.broadcast_to(sin_q[q : q + 1, :], (L, 128))
        cos_ref[q * L : (q + 1) * L, :] = cq * cos_z - sq * sin_z
        sin_ref[q * L : (q + 1) * L, :] = sq * cos_z + cq * sin_z


CHUNKS = ((0, 512), (512, 1024), (1536, 1056))


def wave_of(chunk, vec_ref, wave_ref, cos_ref, sin_ref):
    first, count = CHUNKS[chunk]
    row = first
    while row < first + count:
        site = row % SITES
        rows = min(48, first + count - row, SITES - site)
        at = pl.ds(row, rows)
        cosine = cos_ref[pl.ds(site, rows), :]
        sine = sin_ref[pl.ds(site, rows), :]
        for half in range(2):
            lanes = pl.ds(half * 128, 128)
            lanes_imag = pl.ds(256 + half * 128, 128)
            real = vec_ref[at, lanes].astype(jnp.float32)
            imag = vec_ref[at, lanes_imag].astype(jnp.float32)
            wave_ref[at, lanes] = (cosine * real - sine * imag).astype(jnp.bfloat16)
            wave_ref[at, lanes_imag] = (cosine * imag + sine * real).astype(jnp.bfloat16)
        row += rows


def colour_term(chunk, vec_ref, wave_ref):
    at = pl.ds(*CHUNKS[chunk])
    return lax.dot_general(vec_ref[at, :], wave_ref[at, :], (((0,), (0,)), ((), ())), preferred_element_type=jnp.float32)


def finish_elemental(term, out_ref):
    out_ref[:, 0:256] = term[0:256, 0:256] + term[256:512, 256:512]
    out_ref[:, 256:512] = term[0:256, 256:512] - term[256:512, 0:256]


def kernel(
    sink_hbm, source_hbm, per_hbm, mom_ref, snk_t, src_t,
    out_ref,
    snk_vec, src_vec, wave, wave2, cos_ref, sin_ref, acc,
    snk_part, src_part, per, pt, tbuf,
    y_recv, y_far, y_far_recv, y_sum, z_recv, elem, core_recv, core_sum, x_recv, x_sum, zz_recv, src_elem,
    est, sst, tot,
    load_sem, send_sem, recv_sem,
):
    i = lax.axis_index("tsnk")
    j = lax.axis_index("tsrc")
    x, zh, c = i // 4, (i // 2) % 2, i % 2
    y, zl = j // 4, j % 4
    core_peer = (4 * x + 2 * zh + (1 - c), j)
    z_peer = (4 * x + 2 * (1 - zh) + c, j)
    x_peers = [(4 * ((x + d) % 4) + 2 * zh + c, j) for d in (1, 2, 3)]
    y_peers = [(i, 4 * ((y + d) % 4) + zl) for d in (1, 2, 3)]
    zl_peers = [(i, 4 * y + (zl + d) % 4) for d in (1, 2, 3)]

    def load(n, src, dst):
        return pltpu.make_async_copy(src, dst, load_sem.at[n])

    src_loads = [
        [load(6 + 2 * k + r, source_hbm.at[r, k], src_vec.at[pl.ds(k * SITES, SITES), pl.ds(r * 256, 256)]) for r in range(2)]
        for k in range(COLOURS)
    ]
    snk_loads = [
        [load(2 * k + r, sink_hbm.at[r, k], snk_vec.at[pl.ds(k * SITES, SITES), pl.ds(r * 256, 256)]) for r in range(2)]
        for k in range(COLOURS)
    ]
    per_loads = [load(12 + s, per_hbm.at[s], per.at[s]) for s in range(4)]
    for copies in src_loads:
        for copy in copies:
            copy.start()

    barrier = pltpu.get_barrier_semaphore()
    peers = [core_peer, z_peer] + x_peers + y_peers + zl_peers
    for peer in peers:
        pl.semaphore_signal(barrier, inc=1, device_id=peer, device_id_type=MESH)

    def remote(n, src, dst, peer):
        return pltpu.make_async_remote_copy(
            src_ref=src, dst_ref=dst, send_sem=send_sem.at[n], recv_sem=recv_sem.at[n],
            device_id=peer, device_id_type=MESH,
        )

    def start(copies):
        for copy in copies:
            copy.start()

    def block_of(start_row, size):
        return pl.ds(pl.multiple_of(start_row, size), size)

    def loaded(copies):
        for copy in copies:
            copy.wait()

    phase_tables(mom_ref, i * (SITES // L), cos_ref, sin_ref)
    loaded(src_loads[0])
    wave_of(0, src_vec, wave, cos_ref, sin_ref)
    loaded(src_loads[1])
    for copies in snk_loads:
        start(copies)
    acc[...] = colour_term(0, src_vec, wave)
    wave_of(1, src_vec, wave, cos_ref, sin_ref)
    loaded(src_loads[2])
    acc[...] += colour_term(1, src_vec, wave)
    wave_of(2, src_vec, wave, cos_ref, sin_ref)
    finish_elemental(acc[...] + colour_term(2, src_vec, wave), src_part)
    pl.semaphore_wait(barrier, len(peers))
    core_rs = remote(3, src_part.at[block_of(128 * (1 - c), 128)], core_recv, core_peer)
    core_rs.start()

    start(per_loads)

    phase_tables(mom_ref, j * (SITES // L), cos_ref, sin_ref)
    for colour in range(COLOURS):
        loaded(snk_loads[colour])
    wave_of(0, snk_vec, wave2, cos_ref, sin_ref)
    acc[...] = colour_term(0, snk_vec, wave2)
    wave_of(1, snk_vec, wave2, cos_ref, sin_ref)
    core_rs.wait_recv()
    core_sum[...] = src_part[block_of(128 * c, 128), :] + core_recv[...]
    x_rs = [
        remote(4 + d, core_sum.at[block_of(32 * ((x + d + 1) % 4), 32)], x_recv.at[d], x_peers[d]) for d in range(3)
    ]
    start(x_rs)
    acc[...] += colour_term(1, snk_vec, wave2)
    wave_of(2, snk_vec, wave2, cos_ref, sin_ref)
    finish_elemental(acc[...] + colour_term(2, snk_vec, wave2), snk_part)
    y_far[...] = snk_part[block_of(64 * ((y + 2) % 4), 64), :].astype(jnp.bfloat16)
    y_rs = [
        remote(0, snk_part.at[block_of(64 * ((y + 1) % 4), 64)], y_recv.at[0], y_peers[0]),
        remote(2, snk_part.at[block_of(64 * ((y + 3) % 4), 64)], y_recv.at[1], y_peers[2]),
        remote(1, y_far, y_far_recv, y_peers[1]),
    ]
    start(y_rs)

    out_row = lax.broadcasted_iota(jnp.int32, (256, 256), 0)
    in_row = lax.broadcasted_iota(jnp.int32, (256, 256), 1)
    pick = jnp.where((out_row % 32) * 8 + out_row // 32 == in_row, 1.0, 0.0).astype(jnp.bfloat16)

    def unmix(s, carry):
        per_loads_wait = pltpu.make_async_copy(per_hbm.at[s], per.at[s], load_sem.at[12 + s])
        per_loads_wait.wait()
        for blk in range(8):
            rows = pl.ds(blk * 256, 256)
            both = jnp.concatenate([per[s, 0, rows, :], per[s, 1, rows, :]], axis=1)
            moved = jnp.dot(pick, both, preferred_element_type=jnp.float32).astype(jnp.bfloat16)
            for t in range(4):
                for half in range(2):
                    piece = moved[(half * 4 + t) * 32 : (half * 4 + t + 1) * 32, :]
                    for r in range(2):
                        pt[s, r, t, pl.ds(blk * 32, 32), pl.ds(half * 128, 128)] = piece[
                            :, r * 128 : (r + 1) * 128
                        ]
        return carry

    lax.fori_loop(0, 4, unmix, 0)

    for copy in x_rs:
        copy.wait_recv()
    x_sum[...] = (core_sum[block_of(32 * x, 32), :] + x_recv[0]) + (x_recv[1] + x_recv[2])
    zz = remote(10, x_sum, zz_recv, z_peer)
    zz.start()

    for copy in y_rs:
        copy.wait_recv()
    y_sum[...] = (snk_part[block_of(64 * y, 64), :] + y_recv[0]) + (
        y_recv[1] + y_far_recv[...].astype(jnp.float32)
    )
    z_rs = [
        remote(7 + d, y_sum.at[block_of(16 * ((zl + d + 1) % 4), 16)], z_recv.at[d], zl_peers[d]) for d in range(3)
    ]
    start(z_rs)

    zz.wait_recv()
    src_own = src_elem.at[block_of(128 * c + 32 * x, 32)]
    src_own[...] = (x_sum[...] + zz_recv[...]).astype(jnp.bfloat16)
    x_ag = [remote(26 + d, src_own, src_own, x_peers[d]) for d in range(3)]
    start(x_ag)
    core_ag = [remote(29, src_own, src_own, core_peer)]
    start(core_ag)

    for copy in z_rs:
        copy.wait_recv()
    mine = (y_sum[block_of(16 * zl, 16), :] + z_recv[0]) + (z_recv[1] + z_recv[2])
    own = elem.at[block_of(64 * y + 16 * zl, 16)]
    own[...] = mine.astype(jnp.bfloat16)
    z_ag = [remote(11 + d, own, own, zl_peers[d]) for d in range(3)]
    start(z_ag)
    y_ag = [remote(14 + d, own, own, y_peers[d]) for d in range(3)]
    start(y_ag)

    for d in range(3):
        x_ag[d].wait_recv()
        came = src_elem.at[block_of(128 * c + 32 * ((x + 3 - d) % 4), 32)]
        onward = remote(30 + d, came, came, core_peer)
        onward.start()
        core_ag.append(onward)
    for d in range(3):
        z_ag[d].wait_recv()
        came = elem.at[block_of(64 * y + 16 * ((zl + 3 - d) % 4), 16)]
        onward = [remote(17 + 3 * d + e, came, came, y_peers[e]) for e in range(3)]
        start(onward)
        y_ag += onward
    for copy in core_ag:
        copy.wait_recv()

    sst[0:256, :] = src_elem[...]
    sst[256:512, 0:256] = -src_elem[:, 256:512]
    sst[256:512, 256:512] = src_elem[:, 0:256]

    def right(s, carry):
        rows = jnp.concatenate([pt[s, 0].reshape(1024, 256), pt[s, 1].reshape(1024, 256)], axis=1)
        tbuf[s] = jnp.dot(rows, sst[...], preferred_element_type=jnp.float32).reshape(4, 256, 512)
        return carry

    lax.fori_loop(0, 4, right, 0, unroll=True)

    for copy in y_ag:
        copy.wait_recv()
    est[0:256, 0:256] = elem[:, 0:256]
    est[0:256, 256:512] = -elem[:, 256:512]
    est[256:512, 0:256] = elem[:, 256:512]
    est[256:512, 256:512] = elem[:, 0:256]
    tot[...] = jnp.zeros_like(tot)

    def fold(v):
        return v.reshape(32, 8, 256).sum(axis=0)

    def left(s, carry):
        other = (s + 2) % 4
        sum_real = jnp.zeros((8, 256), jnp.float32)
        sum_imag = jnp.zeros((8, 256), jnp.float32)
        for t in range(4):
            lt = jnp.dot(est[...], jnp.concatenate([pt[s, 0, t], pt[s, 1, t]], axis=0), preferred_element_type=jnp.float32)
            right_real = tbuf[other, t ^ 2, :, 0:256]
            right_imag = tbuf[other, t ^ 2, :, 256:512]
            left_real = lt[0:256]
            left_imag = lt[256:512]
            real = fold(left_real * right_real + left_imag * right_imag)
            imag = fold(left_imag * right_real - left_real * right_imag)
            if t < 2:
                sum_real, sum_imag = sum_real + real, sum_imag + imag
            else:
                sum_real, sum_imag = sum_real - real, sum_imag - imag
        sign = 1.0 - 2.0 * (s // 2).astype(jnp.float32)
        tot[0] += sign * sum_real
        tot[1] += sign * sum_imag
        return carry

    lax.fori_loop(0, 4, left, 0, unroll=True)
    keep = jnp.where(snk_t[0] >= src_t[0], 1.0, 0.0)
    out_ref[0, 0] = jnp.sum(tot[0]) * keep
    out_ref[0, 1] = jnp.sum(tot[1]) * keep

    for copy in y_rs + [core_rs] + x_rs + z_rs + [zz] + z_ag + y_ag + x_ag + core_ag:
        copy.wait_send()


def per_device(sink_vectors, source_vectors, peramb, momenta, sink_times, source_times):
    sink = sink_vectors[0].transpose(0, 2, 3, 1)
    source = source_vectors[0].transpose(0, 2, 3, 1)
    per = peramb[0, 0].reshape(4, 2, 256, 4, 2, 128).transpose(0, 1, 2, 4, 3, 5).reshape(4, 2, 2048, 128)
    hbm = pl.BlockSpec(memory_space=pl.ANY)
    smem = pl.BlockSpec(memory_space=pltpu.SMEM)
    f32, bf16 = jnp.float32, jnp.bfloat16
    values = pl.pallas_call(
        kernel,
        out_shape=jax.ShapeDtypeStruct((1, 2), f32),
        in_specs=[hbm, hbm, hbm, smem, smem, smem],
        out_specs=smem,
        scratch_shapes=[
            pltpu.VMEM((COLOURS * SITES, 512), bf16),
            pltpu.VMEM((COLOURS * SITES, 512), bf16),
            pltpu.VMEM((COLOURS * SITES, 512), bf16),
            pltpu.VMEM((COLOURS * SITES, 512), bf16),
            pltpu.VMEM((SITES, 128), f32),
            pltpu.VMEM((SITES, 128), f32),
            pltpu.VMEM((512, 512), f32),
            pltpu.VMEM((256, 512), f32),
            pltpu.VMEM((256, 512), f32),
            pltpu.VMEM((4, 2, 2048, 128), bf16),
            pltpu.VMEM((4, 2, 4, 256, 256), bf16),
            pltpu.VMEM((4, 4, 256, 512), f32),
            pltpu.VMEM((2, 64, 512), f32),
            pltpu.VMEM((64, 512), bf16),
            pltpu.VMEM((64, 512), bf16),
            pltpu.VMEM((64, 512), f32),
            pltpu.VMEM((3, 16, 512), f32),
            pltpu.VMEM((256, 512), bf16),
            pltpu.VMEM((128, 512), f32),
            pltpu.VMEM((128, 512), f32),
            pltpu.VMEM((3, 32, 512), f32),
            pltpu.VMEM((32, 512), f32),
            pltpu.VMEM((32, 512), f32),
            pltpu.VMEM((256, 512), bf16),
            pltpu.VMEM((512, 512), bf16),
            pltpu.VMEM((512, 512), bf16),
            pltpu.VMEM((2, 8, 256), f32),
            pltpu.SemaphoreType.DMA((16,)),
            pltpu.SemaphoreType.DMA((33,)),
            pltpu.SemaphoreType.DMA((33,)),
        ],
        compiler_params=pltpu.CompilerParams(
            collective_id=0, has_side_effects=True, vmem_limit_bytes=60 * 1024 * 1024
        ),
    )(sink, source, per, momenta, sink_times, source_times)
    return values.reshape(1, 2, 1, 1)


def solution(mesh):
    return jax.shard_map(
        per_device,
        mesh=mesh,
        in_specs=(
            P("tsnk", None, None, None, "tsrc"),
            P("tsrc", None, None, None, "tsnk"),
            P("tsnk", "tsrc", None, None, None, None, None),
            P(),
            P("tsnk"),
            P("tsrc"),
        ),
        out_specs=P(None, None, "tsnk", "tsrc"),
        check_vma=False,
    )
```

```python
import math

import jax
import jax.numpy as jnp
from jax import lax
from jax.experimental import pallas as pl
from jax.experimental.pallas import tpu as pltpu
from jax.sharding import PartitionSpec as P

VECS = 256
L = 24
SITES = 864
COLOURS = 3
MESH = pl.DeviceIdType.MESH
COS = [math.cos(2.0 * math.pi * k / L) for k in range(L)]
SIN = [math.sin(2.0 * math.pi * k / L) for k in range(L)]


def mod_winding(v):
    return v - 24.0 * jnp.floor((v + 0.5) * (1.0 / 24.0))


def cos_sin(k):
    cosine = jnp.zeros_like(k)
    sine = jnp.zeros_like(k)
    for m in range(L):
        hit = k == float(m)
        cosine = jnp.where(hit, COS[m], cosine)
        sine = jnp.where(hit, SIN[m], sine)
    return cosine, sine


def phase_tables(mom_ref, first_row, cos_ref, sin_ref):
    px = mom_ref[0, 0].astype(jnp.float32)
    py = mom_ref[0, 1].astype(jnp.float32)
    pz = mom_ref[0, 2].astype(jnp.float32)
    z = lax.broadcasted_iota(jnp.int32, (L, 128), 0).astype(jnp.float32)
    cos_z, sin_z = cos_sin(mod_winding(pz * z))
    row = (lax.broadcasted_iota(jnp.int32, (40, 128), 0) + first_row).astype(jnp.float32)
    x = jnp.floor((row + 0.5) * (1.0 / L))
    y = row - L * x
    cos_q, sin_q = cos_sin(mod_winding(px * x + py * y))
    for q in range(SITES // L):
        cq = jnp.broadcast_to(cos_q[q : q + 1, :], (L, 128))
        sq = jnp.broadcast_to(sin_q[q : q + 1, :], (L, 128))
        cos_ref[q * L : (q + 1) * L, :] = cq * cos_z - sq * sin_z
        sin_ref[q * L : (q + 1) * L, :] = sq * cos_z + cq * sin_z


CHUNKS = ((0, 256), (256, 1024), (1280, 1312))


def wave_of(chunk, vec_ref, wave_ref, cos_ref, sin_ref):
    first, count = CHUNKS[chunk]
    row = first
    while row < first + count:
        site = row % SITES
        rows = min(48, first + count - row, SITES - site)
        at = pl.ds(row, rows)
        cosine = cos_ref[pl.ds(site, rows), :]
        sine = sin_ref[pl.ds(site, rows), :]
        for half in range(2):
            lanes = pl.ds(half * 128, 128)
            lanes_imag = pl.ds(256 + half * 128, 128)
            real = vec_ref[at, lanes].astype(jnp.float32)
            imag = vec_ref[at, lanes_imag].astype(jnp.float32)
            wave_ref[at, lanes] = (cosine * real - sine * imag).astype(jnp.bfloat16)
            wave_ref[at, lanes_imag] = (cosine * imag + sine * real).astype(jnp.bfloat16)
        row += rows


def colour_term(chunk, vec_ref, wave_ref):
    at = pl.ds(*CHUNKS[chunk])
    return lax.dot_general(vec_ref[at, :], wave_ref[at, :], (((0,), (0,)), ((), ())), preferred_element_type=jnp.float32)


def finish_elemental(term, out_ref):
    out_ref[:, 0:256] = term[0:256, 0:256] + term[256:512, 256:512]
    out_ref[:, 256:512] = term[0:256, 256:512] - term[256:512, 0:256]


def kernel(
    sink_hbm, source_hbm, per_hbm, mom_ref, snk_t, src_t,
    out_ref,
    snk_vec, src_vec, wave, wave2, cos_ref, sin_ref, acc,
    snk_part, src_part, per, pt, tbuf,
    y_recv, y_sum, z_recv, elem, core_recv, core_sum, x_recv, x_sum, zz_recv, src_elem,
    est, sst, tot,
    load_sem, send_sem, recv_sem,
):
    i = lax.axis_index("tsnk")
    j = lax.axis_index("tsrc")
    x, zh, c = i // 4, (i // 2) % 2, i % 2
    y, zl = j // 4, j % 4
    core_peer = (4 * x + 2 * zh + (1 - c), j)
    z_peer = (4 * x + 2 * (1 - zh) + c, j)
    x_peers = [(4 * ((x + d) % 4) + 2 * zh + c, j) for d in (1, 2, 3)]
    y_peers = [(i, 4 * ((y + d) % 4) + zl) for d in (1, 2, 3)]
    zl_peers = [(i, 4 * y + (zl + d) % 4) for d in (1, 2, 3)]

    def load(n, src, dst):
        return pltpu.make_async_copy(src, dst, load_sem.at[n])

    src_loads = [
        [load(6 + 2 * k + r, source_hbm.at[r, k], src_vec.at[pl.ds(k * SITES, SITES), pl.ds(r * 256, 256)]) for r in range(2)]
        for k in range(COLOURS)
    ]
    snk_loads = [
        [load(2 * k + r, sink_hbm.at[r, k], snk_vec.at[pl.ds(k * SITES, SITES), pl.ds(r * 256, 256)]) for r in range(2)]
        for k in range(COLOURS)
    ]
    per_loads = [load(12 + s, per_hbm.at[s], per.at[s]) for s in range(4)]
    for copies in src_loads:
        for copy in copies:
            copy.start()

    barrier = pltpu.get_barrier_semaphore()
    peers = [core_peer, z_peer] + x_peers + y_peers + zl_peers
    for peer in peers:
        pl.semaphore_signal(barrier, inc=1, device_id=peer, device_id_type=MESH)

    def remote(n, src, dst, peer):
        return pltpu.make_async_remote_copy(
            src_ref=src, dst_ref=dst, send_sem=send_sem.at[n], recv_sem=recv_sem.at[n],
            device_id=peer, device_id_type=MESH,
        )

    def start(copies):
        for copy in copies:
            copy.start()

    def block_of(start_row, size):
        return pl.ds(pl.multiple_of(start_row, size), size)

    def loaded(copies):
        for copy in copies:
            copy.wait()

    phase_tables(mom_ref, i * (SITES // L), cos_ref, sin_ref)
    loaded(src_loads[0])
    wave_of(0, src_vec, wave, cos_ref, sin_ref)
    loaded(src_loads[1])
    for copies in snk_loads:
        start(copies)
    acc[...] = colour_term(0, src_vec, wave)
    wave_of(1, src_vec, wave, cos_ref, sin_ref)
    loaded(src_loads[2])
    acc[...] += colour_term(1, src_vec, wave)
    wave_of(2, src_vec, wave, cos_ref, sin_ref)
    finish_elemental(acc[...] + colour_term(2, src_vec, wave), src_part)
    pl.semaphore_wait(barrier, len(peers))
    core_rs = remote(3, src_part.at[block_of(128 * (1 - c), 128)], core_recv, core_peer)
    core_rs.start()

    start(per_loads)

    phase_tables(mom_ref, j * (SITES // L), cos_ref, sin_ref)
    for colour in range(COLOURS):
        loaded(snk_loads[colour])
    wave_of(0, snk_vec, wave2, cos_ref, sin_ref)
    acc[...] = colour_term(0, snk_vec, wave2)
    wave_of(1, snk_vec, wave2, cos_ref, sin_ref)
    acc[...] += colour_term(1, snk_vec, wave2)
    wave_of(2, snk_vec, wave2, cos_ref, sin_ref)
    core_rs.wait_recv()
    core_sum[...] = src_part[block_of(128 * c, 128), :] + core_recv[...]
    x_rs = [
        remote(4 + d, core_sum.at[block_of(32 * ((x + d + 1) % 4), 32)], x_recv.at[d], x_peers[d]) for d in range(3)
    ]
    start(x_rs)
    finish_elemental(acc[...] + colour_term(2, snk_vec, wave2), snk_part)
    y_rs = [
        remote(d, snk_part.at[block_of(64 * ((y + d + 1) % 4), 64)], y_recv.at[d], y_peers[d]) for d in range(3)
    ]
    start(y_rs)

    out_row = lax.broadcasted_iota(jnp.int32, (256, 256), 0)
    in_row = lax.broadcasted_iota(jnp.int32, (256, 256), 1)
    pick = jnp.where((out_row % 32) * 8 + out_row // 32 == in_row, 1.0, 0.0).astype(jnp.bfloat16)

    def unmix(s, carry):
        per_loads_wait = pltpu.make_async_copy(per_hbm.at[s], per.at[s], load_sem.at[12 + s])
        per_loads_wait.wait()
        for blk in range(8):
            rows = pl.ds(blk * 256, 256)
            both = jnp.concatenate([per[s, 0, rows, :], per[s, 1, rows, :]], axis=1)
            moved = jnp.dot(pick, both, preferred_element_type=jnp.float32).astype(jnp.bfloat16)
            for t in range(4):
                for half in range(2):
                    piece = moved[(half * 4 + t) * 32 : (half * 4 + t + 1) * 32, :]
                    for r in range(2):
                        pt[s, r, t, pl.ds(blk * 32, 32), pl.ds(half * 128, 128)] = piece[
                            :, r * 128 : (r + 1) * 128
                        ]
        return carry

    lax.fori_loop(0, 4, unmix, 0)

    for copy in x_rs:
        copy.wait_recv()
    x_sum[...] = (core_sum[block_of(32 * x, 32), :] + x_recv[0]) + (x_recv[1] + x_recv[2])
    zz = remote(10, x_sum, zz_recv, z_peer)
    zz.start()

    for copy in y_rs:
        copy.wait_recv()
    y_sum[...] = (snk_part[block_of(64 * y, 64), :] + y_recv[0]) + (y_recv[1] + y_recv[2])
    z_rs = [
        remote(7 + d, y_sum.at[block_of(16 * ((zl + d + 1) % 4), 16)], z_recv.at[d], zl_peers[d]) for d in range(3)
    ]
    start(z_rs)

    zz.wait_recv()
    src_own = src_elem.at[block_of(128 * c + 32 * x, 32)]
    src_own[...] = (x_sum[...] + zz_recv[...]).astype(jnp.bfloat16)
    x_ag = [remote(26 + d, src_own, src_own, x_peers[d]) for d in range(3)]
    start(x_ag)
    core_ag = [remote(29, src_own, src_own, core_peer)]
    start(core_ag)

    for copy in z_rs:
        copy.wait_recv()
    mine = (y_sum[block_of(16 * zl, 16), :] + z_recv[0]) + (z_recv[1] + z_recv[2])
    own = elem.at[block_of(64 * y + 16 * zl, 16)]
    own[...] = mine.astype(jnp.bfloat16)
    z_ag = [remote(11 + d, own, own, zl_peers[d]) for d in range(3)]
    start(z_ag)
    y_ag = [remote(14 + d, own, own, y_peers[d]) for d in range(3)]
    start(y_ag)

    for d in range(3):
        x_ag[d].wait_recv()
        came = src_elem.at[block_of(128 * c + 32 * ((x + 3 - d) % 4), 32)]
        onward = remote(30 + d, came, came, core_peer)
        onward.start()
        core_ag.append(onward)
    for d in range(3):
        z_ag[d].wait_recv()
        came = elem.at[block_of(64 * y + 16 * ((zl + 3 - d) % 4), 16)]
        onward = [remote(17 + 3 * d + e, came, came, y_peers[e]) for e in range(3)]
        start(onward)
        y_ag += onward
    for copy in core_ag:
        copy.wait_recv()

    sst[0:256, :] = src_elem[...]
    sst[256:512, 0:256] = -src_elem[:, 256:512]
    sst[256:512, 256:512] = src_elem[:, 0:256]

    def right(s, carry):
        rows = jnp.concatenate([pt[s, 0].reshape(1024, 256), pt[s, 1].reshape(1024, 256)], axis=1)
        tbuf[s] = jnp.dot(rows, sst[...], preferred_element_type=jnp.float32).reshape(4, 256, 512)
        return carry

    lax.fori_loop(0, 4, right, 0, unroll=True)

    for copy in y_ag:
        copy.wait_recv()
    est[0:256, 0:256] = elem[:, 0:256]
    est[0:256, 256:512] = -elem[:, 256:512]
    est[256:512, 0:256] = elem[:, 256:512]
    est[256:512, 256:512] = elem[:, 0:256]
    tot[...] = jnp.zeros_like(tot)

    def fold(v):
        return v.reshape(32, 8, 256).sum(axis=0)

    def left(s, carry):
        other = (s + 2) % 4
        sum_real = jnp.zeros((8, 256), jnp.float32)
        sum_imag = jnp.zeros((8, 256), jnp.float32)
        for t in range(4):
            lt = jnp.dot(est[...], jnp.concatenate([pt[s, 0, t], pt[s, 1, t]], axis=0), preferred_element_type=jnp.float32)
            right_real = tbuf[other, t ^ 2, :, 0:256]
            right_imag = tbuf[other, t ^ 2, :, 256:512]
            left_real = lt[0:256]
            left_imag = lt[256:512]
            real = fold(left_real * right_real + left_imag * right_imag)
            imag = fold(left_imag * right_real - left_real * right_imag)
            if t < 2:
                sum_real, sum_imag = sum_real + real, sum_imag + imag
            else:
                sum_real, sum_imag = sum_real - real, sum_imag - imag
        sign = 1.0 - 2.0 * (s // 2).astype(jnp.float32)
        tot[0] += sign * sum_real
        tot[1] += sign * sum_imag
        return carry

    lax.fori_loop(0, 4, left, 0, unroll=True)
    keep = jnp.where(snk_t[0] >= src_t[0], 1.0, 0.0)
    out_ref[0, 0] = jnp.sum(tot[0]) * keep
    out_ref[0, 1] = jnp.sum(tot[1]) * keep

    for copy in y_rs + [core_rs] + x_rs + z_rs + [zz] + z_ag + y_ag + x_ag + core_ag:
        copy.wait_send()


def per_device(sink_vectors, source_vectors, peramb, momenta, sink_times, source_times):
    sink = sink_vectors[0].transpose(0, 2, 3, 1)
    source = source_vectors[0].transpose(0, 2, 3, 1)
    per = peramb[0, 0].reshape(4, 2, 256, 4, 2, 128).transpose(0, 1, 2, 4, 3, 5).reshape(4, 2, 2048, 128)
    hbm = pl.BlockSpec(memory_space=pl.ANY)
    smem = pl.BlockSpec(memory_space=pltpu.SMEM)
    f32, bf16 = jnp.float32, jnp.bfloat16
    values = pl.pallas_call(
        kernel,
        out_shape=jax.ShapeDtypeStruct((1, 2), f32),
        in_specs=[hbm, hbm, hbm, smem, smem, smem],
        out_specs=smem,
        scratch_shapes=[
            pltpu.VMEM((COLOURS * SITES, 512), bf16),
            pltpu.VMEM((COLOURS * SITES, 512), bf16),
            pltpu.VMEM((COLOURS * SITES, 512), bf16),
            pltpu.VMEM((COLOURS * SITES, 512), bf16),
            pltpu.VMEM((SITES, 128), f32),
            pltpu.VMEM((SITES, 128), f32),
            pltpu.VMEM((512, 512), f32),
            pltpu.VMEM((256, 512), f32),
            pltpu.VMEM((256, 512), f32),
            pltpu.VMEM((4, 2, 2048, 128), bf16),
            pltpu.VMEM((4, 2, 4, 256, 256), bf16),
            pltpu.VMEM((4, 4, 256, 512), f32),
            pltpu.VMEM((3, 64, 512), f32),
            pltpu.VMEM((64, 512), f32),
            pltpu.VMEM((3, 16, 512), f32),
            pltpu.VMEM((256, 512), bf16),
            pltpu.VMEM((128, 512), f32),
            pltpu.VMEM((128, 512), f32),
            pltpu.VMEM((3, 32, 512), f32),
            pltpu.VMEM((32, 512), f32),
            pltpu.VMEM((32, 512), f32),
            pltpu.VMEM((256, 512), bf16),
            pltpu.VMEM((512, 512), bf16),
            pltpu.VMEM((512, 512), bf16),
            pltpu.VMEM((2, 8, 256), f32),
            pltpu.SemaphoreType.DMA((16,)),
            pltpu.SemaphoreType.DMA((33,)),
            pltpu.SemaphoreType.DMA((33,)),
        ],
        compiler_params=pltpu.CompilerParams(
            collective_id=0, has_side_effects=True, vmem_limit_bytes=60 * 1024 * 1024
        ),
    )(sink, source, per, momenta, sink_times, source_times)
    return values.reshape(1, 2, 1, 1)


def solution(mesh):
    return jax.shard_map(
        per_device,
        mesh=mesh,
        in_specs=(
            P("tsnk", None, None, None, "tsrc"),
            P("tsrc", None, None, None, "tsnk"),
            P("tsnk", "tsrc", None, None, None, None, None),
            P(),
            P("tsnk"),
            P("tsrc"),
        ),
        out_specs=P(None, None, "tsnk", "tsrc"),
        check_vma=False,
    )
```

```python
import math

import jax
import jax.numpy as jnp
from jax import lax
from jax.experimental import pallas as pl
from jax.experimental.pallas import tpu as pltpu
from jax.sharding import PartitionSpec as P

VECS = 256
L = 24
SITES = 864
COLOURS = 3
MESH = pl.DeviceIdType.MESH
COS = [math.cos(2.0 * math.pi * k / L) for k in range(L)]
SIN = [math.sin(2.0 * math.pi * k / L) for k in range(L)]


def mod_winding(v):
    return v - 24.0 * jnp.floor((v + 0.5) * (1.0 / 24.0))


def cos_sin(k):
    cosine = jnp.zeros_like(k)
    sine = jnp.zeros_like(k)
    for m in range(L):
        hit = k == float(m)
        cosine = jnp.where(hit, COS[m], cosine)
        sine = jnp.where(hit, SIN[m], sine)
    return cosine, sine


def phase_tables(mom_ref, first_row, cos_ref, sin_ref):
    px = mom_ref[0, 0].astype(jnp.float32)
    py = mom_ref[0, 1].astype(jnp.float32)
    pz = mom_ref[0, 2].astype(jnp.float32)
    z = lax.broadcasted_iota(jnp.int32, (L, 128), 0).astype(jnp.float32)
    cos_z, sin_z = cos_sin(mod_winding(pz * z))
    row = (lax.broadcasted_iota(jnp.int32, (40, 128), 0) + first_row).astype(jnp.float32)
    x = jnp.floor((row + 0.5) * (1.0 / L))
    y = row - L * x
    cos_q, sin_q = cos_sin(mod_winding(px * x + py * y))
    for q in range(SITES // L):
        cq = jnp.broadcast_to(cos_q[q : q + 1, :], (L, 128))
        sq = jnp.broadcast_to(sin_q[q : q + 1, :], (L, 128))
        cos_ref[q * L : (q + 1) * L, :] = cq * cos_z - sq * sin_z
        sin_ref[q * L : (q + 1) * L, :] = sq * cos_z + cq * sin_z


CHUNKS = ((0, 256), (256, 1024), (1280, 1312))


def wave_of(chunk, vec_ref, wave_ref, cos_ref, sin_ref):
    first, count = CHUNKS[chunk]
    row = first
    while row < first + count:
        site = row % SITES
        rows = min(48, first + count - row, SITES - site)
        at = pl.ds(row, rows)
        cosine = cos_ref[pl.ds(site, rows), :]
        sine = sin_ref[pl.ds(site, rows), :]
        for half in range(2):
            lanes = pl.ds(half * 128, 128)
            lanes_imag = pl.ds(256 + half * 128, 128)
            real = vec_ref[at, lanes].astype(jnp.float32)
            imag = vec_ref[at, lanes_imag].astype(jnp.float32)
            wave_ref[at, lanes] = (cosine * real - sine * imag).astype(jnp.bfloat16)
            wave_ref[at, lanes_imag] = (cosine * imag + sine * real).astype(jnp.bfloat16)
        row += rows


def colour_term(chunk, vec_ref, wave_ref):
    at = pl.ds(*CHUNKS[chunk])
    return lax.dot_general(vec_ref[at, :], wave_ref[at, :], (((0,), (0,)), ((), ())), preferred_element_type=jnp.float32)


def finish_elemental(term, out_ref):
    out_ref[:, 0:256] = term[0:256, 0:256] + term[256:512, 256:512]
    out_ref[:, 256:512] = term[0:256, 256:512] - term[256:512, 0:256]


def kernel(
    sink_hbm, source_hbm, per_hbm, mom_ref, snk_t, src_t,
    out_ref,
    snk_vec, src_vec, wave, wave2, cos_ref, sin_ref, acc,
    snk_part, src_part, per, pt, tbuf,
    y_recv, y_sum, z_recv, elem, core_recv, core_sum, x_recv, x_sum, zz_recv, src_elem,
    est, sst, tot,
    load_sem, send_sem, recv_sem,
):
    i = lax.axis_index("tsnk")
    j = lax.axis_index("tsrc")
    x, zh, c = i // 4, (i // 2) % 2, i % 2
    y, zl = j // 4, j % 4
    core_peer = (4 * x + 2 * zh + (1 - c), j)
    z_peer = (4 * x + 2 * (1 - zh) + c, j)
    x_peers = [(4 * ((x + d) % 4) + 2 * zh + c, j) for d in (1, 2, 3)]
    y_peers = [(i, 4 * ((y + d) % 4) + zl) for d in (1, 2, 3)]
    zl_peers = [(i, 4 * y + (zl + d) % 4) for d in (1, 2, 3)]

    def load(n, src, dst):
        return pltpu.make_async_copy(src, dst, load_sem.at[n])

    src_loads = [
        [load(6 + 2 * k + r, source_hbm.at[r, k], src_vec.at[pl.ds(k * SITES, SITES), pl.ds(r * 256, 256)]) for r in range(2)]
        for k in range(COLOURS)
    ]
    snk_loads = [
        [load(2 * k + r, sink_hbm.at[r, k], snk_vec.at[pl.ds(k * SITES, SITES), pl.ds(r * 256, 256)]) for r in range(2)]
        for k in range(COLOURS)
    ]
    per_loads = [load(12 + s, per_hbm.at[s], per.at[s]) for s in range(4)]
    for copies in src_loads:
        for copy in copies:
            copy.start()

    barrier = pltpu.get_barrier_semaphore()
    peers = [core_peer, z_peer] + x_peers + y_peers + zl_peers
    for peer in peers:
        pl.semaphore_signal(barrier, inc=1, device_id=peer, device_id_type=MESH)

    def remote(n, src, dst, peer):
        return pltpu.make_async_remote_copy(
            src_ref=src, dst_ref=dst, send_sem=send_sem.at[n], recv_sem=recv_sem.at[n],
            device_id=peer, device_id_type=MESH,
        )

    def start(copies):
        for copy in copies:
            copy.start()

    def block_of(start_row, size):
        return pl.ds(pl.multiple_of(start_row, size), size)

    def loaded(copies):
        for copy in copies:
            copy.wait()

    phase_tables(mom_ref, i * (SITES // L), cos_ref, sin_ref)
    loaded(src_loads[0])
    wave_of(0, src_vec, wave, cos_ref, sin_ref)
    loaded(src_loads[1])
    for copies in snk_loads:
        start(copies)
    acc[...] = colour_term(0, src_vec, wave)
    wave_of(1, src_vec, wave, cos_ref, sin_ref)
    loaded(src_loads[2])
    acc[...] += colour_term(1, src_vec, wave)
    wave_of(2, src_vec, wave, cos_ref, sin_ref)
    finish_elemental(acc[...] + colour_term(2, src_vec, wave), src_part)
    pl.semaphore_wait(barrier, len(peers))
    core_rs = remote(3, src_part.at[block_of(128 * (1 - c), 128)], core_recv, core_peer)
    core_rs.start()

    start(per_loads)

    phase_tables(mom_ref, j * (SITES // L), cos_ref, sin_ref)
    for colour in range(COLOURS):
        loaded(snk_loads[colour])
    wave_of(0, snk_vec, wave2, cos_ref, sin_ref)
    acc[...] = colour_term(0, snk_vec, wave2)
    wave_of(1, snk_vec, wave2, cos_ref, sin_ref)
    acc[...] += colour_term(1, snk_vec, wave2)
    wave_of(2, snk_vec, wave2, cos_ref, sin_ref)
    core_rs.wait_recv()
    core_sum[...] = src_part[block_of(128 * c, 128), :] + core_recv[...]
    x_rs = [
        remote(4 + d, core_sum.at[block_of(32 * ((x + d + 1) % 4), 32)], x_recv.at[d], x_peers[d]) for d in range(3)
    ]
    start(x_rs)
    finish_elemental(acc[...] + colour_term(2, snk_vec, wave2), snk_part)
    y_rs = [
        remote(d, snk_part.at[block_of(64 * ((y + d + 1) % 4), 64)], y_recv.at[d], y_peers[d]) for d in range(3)
    ]
    start(y_rs)

    out_row = lax.broadcasted_iota(jnp.int32, (256, 256), 0)
    in_row = lax.broadcasted_iota(jnp.int32, (256, 256), 1)
    pick = jnp.where((out_row % 32) * 8 + out_row // 32 == in_row, 1.0, 0.0).astype(jnp.bfloat16)

    def unmix(s, carry):
        per_loads_wait = pltpu.make_async_copy(per_hbm.at[s], per.at[s], load_sem.at[12 + s])
        per_loads_wait.wait()
        for blk in range(8):
            rows = pl.ds(blk * 256, 256)
            both = jnp.concatenate([per[s, 0, rows, :], per[s, 1, rows, :]], axis=1)
            moved = jnp.dot(pick, both, preferred_element_type=jnp.float32).astype(jnp.bfloat16)
            for t in range(4):
                for half in range(2):
                    piece = moved[(half * 4 + t) * 32 : (half * 4 + t + 1) * 32, :]
                    for r in range(2):
                        pt[s, r, t, pl.ds(blk * 32, 32), pl.ds(half * 128, 128)] = piece[
                            :, r * 128 : (r + 1) * 128
                        ]
        return carry

    lax.fori_loop(0, 4, unmix, 0)

    for copy in x_rs:
        copy.wait_recv()
    x_sum[...] = (core_sum[block_of(32 * x, 32), :] + x_recv[0]) + (x_recv[1] + x_recv[2])
    zz = remote(10, x_sum, zz_recv, z_peer)
    zz.start()

    for copy in y_rs:
        copy.wait_recv()
    y_sum[...] = (snk_part[block_of(64 * y, 64), :] + y_recv[0]) + (y_recv[1] + y_recv[2])
    z_rs = [
        remote(7 + d, y_sum.at[block_of(16 * ((zl + d + 1) % 4), 16)], z_recv.at[d], zl_peers[d]) for d in range(3)
    ]
    start(z_rs)

    zz.wait_recv()
    src_own = src_elem.at[block_of(128 * c + 32 * x, 32)]
    src_own[...] = (x_sum[...] + zz_recv[...]).astype(jnp.bfloat16)
    x_ag = [remote(26 + d, src_own, src_own, x_peers[d]) for d in range(3)]
    start(x_ag)
    core_ag = [remote(29, src_own, src_own, core_peer)]
    start(core_ag)

    for copy in z_rs:
        copy.wait_recv()
    mine = (y_sum[block_of(16 * zl, 16), :] + z_recv[0]) + (z_recv[1] + z_recv[2])
    own = elem.at[block_of(64 * y + 16 * zl, 16)]
    own[...] = mine.astype(jnp.bfloat16)
    z_ag = [remote(11 + d, own, own, zl_peers[d]) for d in range(3)]
    start(z_ag)
    y_ag = [remote(14 + d, own, own, y_peers[d]) for d in range(3)]
    start(y_ag)

    for d in range(3):
        z_ag[d].wait_recv()
        came = elem.at[block_of(64 * y + 16 * ((zl + 3 - d) % 4), 16)]
        onward = [remote(17 + 3 * d + e, came, came, y_peers[e]) for e in range(3)]
        start(onward)
        y_ag += onward
    for d in range(3):
        x_ag[d].wait_recv()
        came = src_elem.at[block_of(128 * c + 32 * ((x + 3 - d) % 4), 32)]
        onward = remote(30 + d, came, came, core_peer)
        onward.start()
        core_ag.append(onward)
    for copy in core_ag:
        copy.wait_recv()

    sst[0:256, :] = src_elem[...]
    sst[256:512, 0:256] = -src_elem[:, 256:512]
    sst[256:512, 256:512] = src_elem[:, 0:256]

    def right(s, carry):
        rows = jnp.concatenate([pt[s, 0].reshape(1024, 256), pt[s, 1].reshape(1024, 256)], axis=1)
        tbuf[s] = jnp.dot(rows, sst[...], preferred_element_type=jnp.float32).reshape(4, 256, 512)
        return carry

    lax.fori_loop(0, 4, right, 0, unroll=True)

    for copy in y_ag:
        copy.wait_recv()
    est[0:256, 0:256] = elem[:, 0:256]
    est[0:256, 256:512] = -elem[:, 256:512]
    est[256:512, 0:256] = elem[:, 256:512]
    est[256:512, 256:512] = elem[:, 0:256]
    tot[...] = jnp.zeros_like(tot)

    def fold(v):
        return v.reshape(32, 8, 256).sum(axis=0)

    def left(s, carry):
        other = (s + 2) % 4
        sum_real = jnp.zeros((8, 256), jnp.float32)
        sum_imag = jnp.zeros((8, 256), jnp.float32)
        for t in range(4):
            lt = jnp.dot(est[...], jnp.concatenate([pt[s, 0, t], pt[s, 1, t]], axis=0), preferred_element_type=jnp.float32)
            right_real = tbuf[other, t ^ 2, :, 0:256]
            right_imag = tbuf[other, t ^ 2, :, 256:512]
            left_real = lt[0:256]
            left_imag = lt[256:512]
            real = fold(left_real * right_real + left_imag * right_imag)
            imag = fold(left_imag * right_real - left_real * right_imag)
            if t < 2:
                sum_real, sum_imag = sum_real + real, sum_imag + imag
            else:
                sum_real, sum_imag = sum_real - real, sum_imag - imag
        sign = 1.0 - 2.0 * (s // 2).astype(jnp.float32)
        tot[0] += sign * sum_real
        tot[1] += sign * sum_imag
        return carry

    lax.fori_loop(0, 4, left, 0, unroll=True)
    keep = jnp.where(snk_t[0] >= src_t[0], 1.0, 0.0)
    out_ref[0, 0] = jnp.sum(tot[0]) * keep
    out_ref[0, 1] = jnp.sum(tot[1]) * keep

    for copy in y_rs + [core_rs] + x_rs + z_rs + [zz] + z_ag + y_ag + x_ag + core_ag:
        copy.wait_send()


def per_device(sink_vectors, source_vectors, peramb, momenta, sink_times, source_times):
    sink = sink_vectors[0].transpose(0, 2, 3, 1)
    source = source_vectors[0].transpose(0, 2, 3, 1)
    per = peramb[0, 0].reshape(4, 2, 256, 4, 2, 128).transpose(0, 1, 2, 4, 3, 5).reshape(4, 2, 2048, 128)
    hbm = pl.BlockSpec(memory_space=pl.ANY)
    smem = pl.BlockSpec(memory_space=pltpu.SMEM)
    f32, bf16 = jnp.float32, jnp.bfloat16
    values = pl.pallas_call(
        kernel,
        out_shape=jax.ShapeDtypeStruct((1, 2), f32),
        in_specs=[hbm, hbm, hbm, smem, smem, smem],
        out_specs=smem,
        scratch_shapes=[
            pltpu.VMEM((COLOURS * SITES, 512), bf16),
            pltpu.VMEM((COLOURS * SITES, 512), bf16),
            pltpu.VMEM((COLOURS * SITES, 512), bf16),
            pltpu.VMEM((COLOURS * SITES, 512), bf16),
            pltpu.VMEM((SITES, 128), f32),
            pltpu.VMEM((SITES, 128), f32),
            pltpu.VMEM((512, 512), f32),
            pltpu.VMEM((256, 512), f32),
            pltpu.VMEM((256, 512), f32),
            pltpu.VMEM((4, 2, 2048, 128), bf16),
            pltpu.VMEM((4, 2, 4, 256, 256), bf16),
            pltpu.VMEM((4, 4, 256, 512), f32),
            pltpu.VMEM((3, 64, 512), f32),
            pltpu.VMEM((64, 512), f32),
            pltpu.VMEM((3, 16, 512), f32),
            pltpu.VMEM((256, 512), bf16),
            pltpu.VMEM((128, 512), f32),
            pltpu.VMEM((128, 512), f32),
            pltpu.VMEM((3, 32, 512), f32),
            pltpu.VMEM((32, 512), f32),
            pltpu.VMEM((32, 512), f32),
            pltpu.VMEM((256, 512), bf16),
            pltpu.VMEM((512, 512), bf16),
            pltpu.VMEM((512, 512), bf16),
            pltpu.VMEM((2, 8, 256), f32),
            pltpu.SemaphoreType.DMA((16,)),
            pltpu.SemaphoreType.DMA((33,)),
            pltpu.SemaphoreType.DMA((33,)),
        ],
        compiler_params=pltpu.CompilerParams(
            collective_id=0, has_side_effects=True, vmem_limit_bytes=60 * 1024 * 1024
        ),
    )(sink, source, per, momenta, sink_times, source_times)
    return values.reshape(1, 2, 1, 1)


def solution(mesh):
    return jax.shard_map(
        per_device,
        mesh=mesh,
        in_specs=(
            P("tsnk", None, None, None, "tsrc"),
            P("tsrc", None, None, None, "tsnk"),
            P("tsnk", "tsrc", None, None, None, None, None),
            P(),
            P("tsnk"),
            P("tsrc"),
        ),
        out_specs=P(None, None, "tsnk", "tsrc"),
        check_vma=False,
    )
```
